512 devices in a mesh: cand: 64 (over z, x), env: 8 (over y, core).
Axes of the slice: x: 4, y: 4, z: 16, core: 2. Of those that a mesh axis runs over, the one named last changes fastest.
Arguments:
- plan_mean: float32 [512, 512], P(('env', 'cand')), parts along dimension 0, may hold values from -0.5 to 0.5
- plan_var: float32 [512, 512], P(('env', 'cand')), parts along dimension 0, may hold values from 0.04 to 0.64
- start_state: float32 [512, 128], P(('env', 'cand')), parts along dimension 0, may hold values from -6 to 6
- noise: bfloat16 [512, 512, 512], P('env', 'cand'), parts along dimension 0, may hold values from -6 to 6
- elite_index: int32 [512, 64], P('env'), parts along dimension 0, may hold values from 0 to 511, as said below
- w_state: bfloat16 [4, 128, 512], replicated, may hold values from -0.5 to 0.5
- w_act: bfloat16 [4, 32, 512], replicated, may hold values from -1 to 1
- bias_hidden: float32 [4, 512], replicated, may hold values from -3 to 3
- w_out: bfloat16 [4, 512, 128], replicated, may hold values from -0.125 to 0.125
Outputs:
- returns: float32 [512, 512], P('env', 'cand'), parts along dimension 0
- new_mean: float32 [512, 512], P(('env', 'cand')), parts along dimension 0
- new_var: float32 [512, 512], P(('env', 'cand')), parts along dimension 0
The draws below stay inside these ranges and needn't reach their ends.
There are 8 independent parts, one for each index of `env`. The reference program is written for one: setup_inputs(seed, part) draws one part's arguments, and reference() takes and returns one part's arrays. A program takes and returns all parts, laid end to end along the dimension named above; an argument that names none is the same for every part. Nothing has to cross between parts.
Inputs may be any that keep to these rules, and one draw needn't show every extreme that they name: `elite_index`: row e lists 64 different candidates of environment e. Among the candidates 8 * b to 8 * (b + 1) - 1 of one environment at most 4 are listed, and in every environment some such block holds exactly 4.
All inputs are finite; a program needn't handle non-finite values.
Results may differ from the reference program's by a relative error of at most 0.0012.
Values may be sent and summed in bfloat16 or wider, within the bound.
A program may use at most 64 MiB of HBM per device.

```python
import math
import jax
import jax.numpy as jnp
from jax import lax

S = 128
ADIM = 32
HID = 512
MEMBERS = 4
HOR = 16
CANDS = 512
ELITE = 64
F = 512
ENV_PART = 64
CAND_DEV = 8
CAP = 4


def draw_elite_index(key, part):
    subkeys = jax.random.split(jax.random.fold_in(key, 17), 3)
    blocks = CANDS // CAND_DEV
    jitter = jax.random.randint(subkeys[0], (ENV_PART, CANDS), 0, 65536)
    block_bias = jax.random.randint(subkeys[1], (ENV_PART, blocks), 0, 3)
    forced_block = jax.random.randint(subkeys[2], (ENV_PART,), 0, blocks)
    block_bias = jnp.where(jnp.arange(blocks)[None, :] == forced_block[:, None], 4, block_bias)
    scores = (jnp.repeat(block_bias, CAND_DEV, axis=1) * 65536 + jitter) * CANDS + jnp.arange(CANDS, dtype=jnp.int32)[None, :]
    block_grid = scores.reshape(ENV_PART, blocks, CAND_DEV)
    order_rank = jnp.sum((block_grid[:, :, None, :] > block_grid[:, :, :, None]).astype(jnp.int32), axis=-1)
    eligible = (order_rank < CAP).reshape(ENV_PART, CANDS)
    capped = jnp.where(eligible, scores, -1)
    return lax.top_k(capped, ELITE)[1].astype(jnp.int32)


def block_scale(rng, dims, pieces, smallest, high):
    def one(dim, parts):
        heights = jax.random.uniform(jax.random.fold_in(jax.random.fold_in(rng, 6), dim), (parts,), jnp.float32, smallest / len(pieces), high / len(pieces))
        return jnp.repeat(jnp.exp(heights), dims[dim] // parts).reshape((-1,) + (1,) * (len(dims) - dim - 1))

    gain = one(*pieces[0])
    for cut in pieces[1:]:
        gain = gain * one(*cut)
    return gain


def normal_values(own_key, shape, width, reach, cuts=(), kind=jnp.bfloat16):
    entries = jax.random.normal(own_key, shape, jnp.float32) * width
    if len(cuts) > 0:
        entries = block_scale(own_key, shape, cuts, -0.22, 0.18) * entries
    return jnp.clip(entries, min=-reach, max=reach).astype(kind)


def setup_inputs(seed: int = 0, part: int = 0) -> dict:
    key_list = jax.random.split(jax.random.key(seed), 10)
    part_splits = jax.random.split(jax.random.fold_in(key_list[9], part), 10)
    return {
        "plan_mean": jnp.clip(jax.random.uniform(part_splits[0], (ENV_PART, F), jnp.float32, -0.5, 0.5) * block_scale(part_splits[0], (ENV_PART, F), ((0, 64),), -0.4, 0.0), -0.5, 0.5),
        "plan_var": jnp.clip(jnp.exp(math.log(0.64) - 2.7725887 * jax.random.uniform(part_splits[1], (ENV_PART, F), jnp.float32) ** block_scale(part_splits[1], (ENV_PART, F), ((0, 64),), -0.2, 0.2)), 0.04, 0.64),
        "start_state": normal_values(part_splits[2], (ENV_PART, S), 1.0, 6.0, ((0, 64),), jnp.float32),
        "noise": normal_values(part_splits[3], (ENV_PART, CANDS, F), 1.0, 6.0, ((1, 64),)),
        "elite_index": draw_elite_index(jax.random.fold_in(jax.random.fold_in(key_list[9], part), 71), part),
        "w_state": normal_values(key_list[5], (MEMBERS, S, HID), S ** -0.5, 0.5),
        "w_act": normal_values(key_list[6], (MEMBERS, ADIM, HID), ADIM ** -0.5, 1.0),
        "bias_hidden": normal_values(key_list[7], (MEMBERS, HID), 0.5, 3.0, (), jnp.float32),
        "w_out": normal_values(key_list[8], (MEMBERS, HID, S), (4 * HID) ** -0.5, 0.125),
    }


ALPHA = 0.1
EPSILON = 1e-06

def rollout(actions, start_state, w_state, w_act, bias_hidden, w_out):
    env_count = actions.shape[0]
    cand_count = actions.shape[1]
    groups = cand_count // MEMBERS
    states = jnp.broadcast_to(start_state[:, None, :], (env_count, cand_count, S)).astype(jnp.float32)
    running = jnp.zeros((env_count, cand_count), jnp.float32)
    hi = lax.Precision.HIGHEST

    def advance(step_index, loop_state):
        states, running = loop_state
        step_act = lax.dynamic_slice_in_dim(actions, (step_index * ADIM).astype(jnp.int32), ADIM, 2)
        energy = lax.optimization_barrier(jnp.mean(states * states, axis=-1, keepdims=True)) + EPSILON
        normed = (states * lax.rsqrt(energy)).astype(jnp.bfloat16)
        grouped = normed.reshape(env_count, groups, MEMBERS, S).astype(jnp.float32)
        act_grouped = step_act.reshape(env_count, groups, MEMBERS, ADIM).astype(jnp.float32)
        preact = jnp.einsum('egms,msh->egmh', grouped, w_state.astype(jnp.float32), precision=hi)
        preact = preact + jnp.einsum('egma,mah->egmh', act_grouped, w_act.astype(jnp.float32), precision=hi)
        preact = preact + bias_hidden[None, None, :, :]
        hidden = jax.nn.silu(preact).astype(jnp.bfloat16)
        change = jnp.einsum('egmh,mhs->egms', hidden.astype(jnp.float32), w_out.astype(jnp.float32), precision=hi)
        states = states + change.reshape(env_count, cand_count, S)
        act_float = step_act.astype(jnp.float32)
        reward = -lax.optimization_barrier(jnp.mean(states * states, axis=-1)) - 0.1 * lax.optimization_barrier(jnp.mean(act_float * act_float, axis=-1))
        return (states, running + reward)
    states, running = lax.fori_loop(0, HOR, advance, (states, running))
    return running / HOR

def reference(plan_mean, plan_var, start_state, noise, elite_index, w_state, w_act, bias_hidden, w_out):
    actions = jnp.clip(plan_mean[:, None, :] + jnp.sqrt(plan_var)[:, None, :] * noise.astype(jnp.float32), -1.0, 1.0).astype(jnp.bfloat16)
    returns = rollout(actions, start_state, w_state, w_act, bias_hidden, w_out)
    elites = jnp.take_along_axis(actions, elite_index.astype(jnp.int32)[:, :, None], axis=1).astype(jnp.float32)
    first_sum = lax.optimization_barrier(jnp.sum(elites, axis=1))
    second_sum = lax.optimization_barrier(jnp.sum(elites * elites, axis=1))
    elite_mean = first_sum / ELITE
    elite_var = second_sum / ELITE - elite_mean * elite_mean
    new_mean = ALPHA * plan_mean + (1.0 - ALPHA) * elite_mean
    new_var = ALPHA * plan_var + (1.0 - ALPHA) * elite_var
    return (returns, new_mean, new_var)
```

```python
import functools

import jax
import jax.numpy as jnp
from jax import lax
from jax.experimental import pallas as pl
from jax.experimental.pallas import tpu as pltpu
from jax.sharding import PartitionSpec as P

BF = jnp.bfloat16
F32 = jnp.float32
ALPHA = 0.1
EPSILON = 1e-06
NX, NZ = 4, 16
ELITE, CAP, CD = 64, 4, 8
S, ADIM, HID, F, M, HOR = 128, 32, 512, 512, 4, 16
E = NX * NZ
ROW = 2 * F + S
NEAR = (1, 15, 2, 14, 3, 13, 4, 12, 5, 11, 6, 10, 7, 9, 8)


def kernel(
    mean_ref, var_ref, start_ref, noise_hbm, elite_ref, ws_hbm, wa_hbm, bias_ref, wo_hbm,
    ret_ref, nm_ref, nv_ref,
    rows, noise_v, noise_f, wide, eip, elites, arrived, sums, parts, w1, w2, act, states, energy,
    asum, perm,
    load_sem, zs, zr, xs, xr, ns, nr, ss, sr,
):
    me = lax.axis_index("cand")
    z, x = me // NX, me % NX

    def zpeer(d):
        return {"cand": ((z + d) % NZ) * NX + x}

    def xpeer(j):
        return {"cand": z * NX + (x + j) % NX}

    def remote(src, dst, send, recv, peer):
        return pltpu.make_async_remote_copy(
            src_ref=src, dst_ref=dst, send_sem=send, recv_sem=recv,
            device_id=peer, device_id_type=pl.DeviceIdType.MESH,
        )

    barrier = pltpu.get_barrier_semaphore()
    for d in NEAR[::-1]:
        pl.semaphore_signal(barrier, inc=1, device_id=zpeer(d), device_id_type=pl.DeviceIdType.MESH)
    for j in range(1, NX):
        pl.semaphore_signal(barrier, inc=1, device_id=xpeer(j), device_id_type=pl.DeviceIdType.MESH)

    loads = [pltpu.make_async_copy(noise_hbm, noise_v, load_sem.at[0])]
    for m in range(M):
        loads.append(pltpu.make_async_copy(wo_hbm.at[m], w2.at[m], load_sem.at[1 + m]))
        for r in range(4):
            n = 5 + 8 * m + 2 * r
            loads.append(
                pltpu.make_async_copy(ws_hbm.at[m], w1.at[m, r, pl.ds(0, S), :], load_sem.at[n])
            )
            loads.append(
                pltpu.make_async_copy(
                    wa_hbm.at[m], w1.at[m, r, pl.ds(S + ADIM * r, ADIM), :], load_sem.at[n + 1]
                )
            )
    for c in loads:
        c.start()

    rows[x, z, :, 0:F] = mean_ref[...]
    rows[x, z, :, F : 2 * F] = jnp.sqrt(var_ref[...])
    rows[x, z, :, 2 * F : ROW] = start_ref[...]

    for m in range(M):
        b = bias_ref[m : m + 1, :]
        hi = b.astype(BF).astype(F32)
        mid = (b - hi).astype(BF).astype(F32)
        low = b - hi - mid
        at = lax.broadcasted_iota(jnp.int32, (ADIM, HID), 0)
        tile = jnp.where(at == 0, hi, jnp.where(at == 1, mid, jnp.where(at == 2, low, 0.0)))
        tile = tile.astype(BF)
        for r in range(4):
            for k in range(4):
                if k != r:
                    w1[m, r, S + ADIM * k : S + ADIM * (k + 1), :] = (
                        tile if k == (r + 1) % 4 else jnp.zeros((ADIM, HID), BF)
                    )

    wide[...] = jnp.full((E, 128), -1, jnp.int32)
    wide[:, 0:ELITE] = elite_ref[...]
    for k in range(NX):
        eip[NZ * k : NZ * (k + 1), :] = wide[pl.ds(k, NZ, stride=NX), :]
    listed = eip[...]
    first = me * CD
    chosen = [
        jnp.sum(jnp.where(listed == first + c, 1.0, 0.0), axis=1, keepdims=True) for c in range(CD)
    ]
    ranks, total = [], jnp.zeros((E, 1), F32)
    for c in range(CD):
        ranks.append(total)
        total = total + chosen[c]

    loads[0].wait()
    for q in range(4):
        part = noise_v[:, :, 128 * q : 128 * (q + 1)]
        noise_f[q] = part.astype(F32).reshape(E * CD, 128)

    def drawn_by(k, c):
        at = pl.ds(k * CD + c, NZ, stride=NX * CD)
        return jnp.concatenate([noise_f[q, at, :] for q in range(4)], axis=1)

    for k in range(NX):
        for s in range(CAP):
            slot = jnp.zeros((NZ, F), F32)
            for c in range(s, CD):
                cut = slice(NZ * k, NZ * (k + 1))
                pick = jnp.where(ranks[c][cut] == float(s), chosen[c][cut], 0.0)
                slot = slot + pick * drawn_by(k, c)
            elites[k, s] = slot.astype(BF)

    pl.semaphore_wait(barrier, NZ - 1 + NX - 1)

    mine = rows.at[x, z]
    z_out = [remote(mine, mine, zs.at[d], zr.at[d], zpeer(d)) for d in NEAR[::-1]]
    for c in z_out:
        c.start()
    x_out = []
    for j in range(1, NX):
        x_out.append(remote(mine, mine, xs.at[0, j], xr.at[0, j], xpeer(j)))
        x_out[-1].start()
    n_out = []
    for j in range(1, NX):
        n_out.append(
            remote(elites.at[(x + j) % NX], arrived.at[j], ns.at[j], nr.at[j], xpeer(j))
        )
        n_out[-1].start()

    for d in NEAR:
        got = rows.at[x, (z - d + NZ) % NZ]
        remote(got, got, zs.at[d], zr.at[d], zpeer(d)).wait_recv()
        for j in range(1, NX):
            x_out.append(remote(got, got, xs.at[d, j], xr.at[d, j], xpeer(j)))
            x_out[-1].start()

    own = rows[x].reshape(NZ, ROW)
    line_mean, line_std = own[:, 0:F], own[:, F : 2 * F]
    line_listed = eip[pl.ds(pl.multiple_of(x * NZ, NZ), NZ), :] // CD
    first_sum = jnp.zeros((NZ, F), F32)
    second_sum = jnp.zeros((NZ, F), F32)
    for j in range(NX):
        block = z * NX + (x - j + NX) % NX
        count = jnp.sum(jnp.where(line_listed == block, 1.0, 0.0), axis=1, keepdims=True)
        if j > 0:
            n_out[j - 1].wait_recv()
        for s in range(CAP):
            drawn = (elites[x, s] if j == 0 else arrived[j, s]).astype(F32)
            a = jnp.clip(line_mean + line_std * drawn, -1.0, 1.0).astype(BF).astype(F32)
            a = jnp.where(count > float(s), a, 0.0)
            first_sum = first_sum + a
            second_sum = second_sum + a * a
    for k in range(4):
        cut = slice(128 * k, 128 * (k + 1))
        sums[pl.ds(k, NZ, stride=8), :] = first_sum[:, cut]
        sums[pl.ds(4 + k, NZ, stride=8), :] = second_sum[:, cut]

    def sum_copy(d):
        return remote(
            sums.at[pl.ds(pl.multiple_of(((z + d) % NZ) * 8, 8), 8), :],
            parts.at[pl.ds(8 * d, 8), :],
            ss.at[d], sr.at[d], zpeer(d),
        )

    s_out = [sum_copy(d) for d in NEAR[::-1]]
    for c in s_out:
        c.start()

    for d in (0,) + NEAR:
        for j in range(1, NX):
            got = rows.at[(x - j + NX) % NX, (z - d + NZ) % NZ]
            remote(got, got, xs.at[d, j], xr.at[d, j], xpeer(j)).wait_recv()

    gathered = [rows[k].reshape(NZ, ROW) for k in range(NX)]
    full_mean = jnp.concatenate([g[:, 0:F] for g in gathered], axis=0)
    full_std = jnp.concatenate([g[:, F : 2 * F] for g in gathered], axis=0)
    full_start = jnp.concatenate([g[:, 2 * F : ROW] for g in gathered], axis=0)
    for c in range(CD):
        m, h = c % M, c // M
        drawn = jnp.concatenate(
            [drawn_by(k, c) for k in range(NX)], axis=0
        )
        a = jnp.clip(full_mean + full_std * drawn, -1.0, 1.0).astype(BF).astype(F32)
        half = (0.5 * a).astype(BF)
        for q in range(4):
            act[m, q, E * h : E * (h + 1), :] = half[:, 128 * q : 128 * (q + 1)]
        asum[m, E * h : E * (h + 1), :] = jnp.sum(a * a, axis=1, keepdims=True)
        states[m, E * h : E * (h + 1), :] = full_start

    for c in loads[1:]:
        c.wait()
    lane = lax.broadcasted_iota(jnp.int32, (2 * E, 128), 1)

    def squares(s):
        return jnp.sum(s * s, axis=1, keepdims=True)

    def step(q, r):
        left = []
        for m in range(M):
            s = states[m]
            e = squares(s)
            energy[m] = energy[m] + e
            n = (s * (0.5 * lax.rsqrt(e * (1.0 / S) + EPSILON))).astype(BF)
            at = ADIM * ((r + 1) % 4)
            ones = jnp.where((lane >= at) & (lane < at + 3), 0.5, 0.0).astype(BF)
            now = (lane >= ADIM * r) & (lane < ADIM * (r + 1))
            left.append((s, jnp.concatenate([n, jnp.where(now, act[m, q], ones)], axis=1)))
        halves = [
            jnp.dot(left[m][1], w1[m, r], preferred_element_type=F32) for m in range(M)
        ]
        for m in range(M):
            h = halves[m]
            hidden = (h + h * jnp.tanh(h)).astype(BF)
            states[m] = left[m][0] + jnp.dot(hidden, w2[m], preferred_element_type=F32)

    initial = squares(full_start)
    for m in range(M):
        energy[m] = -jnp.concatenate([initial, initial], axis=0)

    def quarter(q, carry):
        for r in range(4):
            step(q, r)
        return carry

    lax.fori_loop(0, 4, quarter, 0)

    out_lane = lax.broadcasted_iota(jnp.int32, (E, 128), 1)
    table = jnp.zeros((E, 128), F32)
    for c in range(CD):
        m, h = c % M, c // M
        cut = slice(E * h, E * (h + 1))
        e = energy[m, cut, :] + squares(states[m, cut, :])
        value = e * (-1.0 / (S * HOR)) - asum[m, cut, :] * (0.1 / (ADIM * HOR))
        table = jnp.where(out_lane == c, value, table)
    for k in range(NX):
        perm[pl.ds(k, NZ, stride=NX), :] = table[NZ * k : NZ * (k + 1), :]
    ret_ref[...] = perm[:, 0:CD]

    total = sums[pl.ds(pl.multiple_of(z * 8, 8), 8), :]
    for d in NEAR:
        sum_copy(d).wait_recv()
        total = total + parts[8 * d : 8 * (d + 1), :]
    for k in range(4):
        cut = slice(128 * k, 128 * (k + 1))
        elite_mean = total[k : k + 1, :] * (1.0 / ELITE)
        elite_var = total[4 + k : 5 + k, :] * (1.0 / ELITE) - elite_mean * elite_mean
        nm_ref[:, cut] = ALPHA * mean_ref[:, cut] + (1.0 - ALPHA) * elite_mean
        nv_ref[:, cut] = ALPHA * var_ref[:, cut] + (1.0 - ALPHA) * elite_var

    for c in z_out + x_out + n_out + s_out:
        c.wait_send()


def per_device(mean, var, start, noise, elite, w_state, w_act, bias, w_out):
    vmem = pl.BlockSpec(memory_space=pltpu.VMEM)
    hbm = pl.BlockSpec(memory_space=pl.ANY)
    dma = pltpu.SemaphoreType.DMA
    return pl.pallas_call(
        kernel,
        out_shape=(
            jax.ShapeDtypeStruct((E, CD), F32),
            jax.ShapeDtypeStruct((1, F), F32),
            jax.ShapeDtypeStruct((1, F), F32),
        ),
        in_specs=[vmem, vmem, vmem, hbm, vmem, hbm, hbm, vmem, hbm],
        out_specs=(vmem, vmem, vmem),
        scratch_shapes=[
            pltpu.VMEM((NX, NZ, 1, ROW), F32),
            pltpu.VMEM((E, CD, F), BF),
            pltpu.VMEM((4, E * CD, 128), F32),
            pltpu.VMEM((E, 128), jnp.int32),
            pltpu.VMEM((E, 128), jnp.int32),
            pltpu.VMEM((NX, CAP, NZ, F), BF),
            pltpu.VMEM((NX, CAP, NZ, F), BF),
            pltpu.VMEM((NZ * 8, 128), F32),
            pltpu.VMEM((NZ * 8, 128), F32),
            pltpu.VMEM((M, 4, 2 * S, HID), BF),
            pltpu.VMEM((M, HID, S), BF),
            pltpu.VMEM((M, 4, 2 * E, 128), BF),
            pltpu.VMEM((M, 2 * E, S), F32),
            pltpu.VMEM((M, 2 * E, 1), F32),
            pltpu.VMEM((M, 2 * E, 1), F32),
            pltpu.VMEM((E, 128), F32),
            dma((37,)), dma((NZ,)), dma((NZ,)), dma((NZ, NX)), dma((NZ, NX)),
            dma((NX,)), dma((NX,)), dma((NZ,)), dma((NZ,)),
        ],
        compiler_params=pltpu.CompilerParams(
            collective_id=0, has_side_effects=True, vmem_limit_bytes=48 * 2**20
        ),
    )(mean, var, start, noise, elite, w_state, w_act, bias, w_out)


def solution(mesh):
    both = P(("env", "cand"), None)
    in_specs = (both, both, both, P("env", "cand", None), P("env", None), P(), P(), P(), P())
    return jax.shard_map(
        per_device, mesh=mesh, in_specs=in_specs, out_specs=(P("env", "cand"), both, both),
        check_vma=False,
    )
```

```python
import functools

import jax
import jax.numpy as jnp
from jax import lax
from jax.experimental import pallas as pl
from jax.experimental.pallas import tpu as pltpu
from jax.sharding import PartitionSpec as P

BF = jnp.bfloat16
F32 = jnp.float32
ALPHA = 0.1
EPSILON = 1e-06
NX, NZ = 4, 16
ELITE, CAP, CD = 64, 4, 8
S, ADIM, HID, F, M, HOR = 128, 32, 512, 512, 4, 16
E = NX * NZ
ROW = 2 * F + S
REACH = 4
DIRECT = (1, 15, 2, 14, 3, 13, 4, 12)
RELAYED = (5, 11, 6, 10, 7, 9, 8)
NEAR = DIRECT + RELAYED


def kernel(
    mean_hbm, var_hbm, start_hbm, noise_hbm, elite_hbm, ws_hbm, wa_hbm, bias_hbm, wo_hbm,
    ret_ref, nm_ref, nv_ref,
    mean_ref, var_ref, start_ref, elite_ref, bias_ref, rows, noise_v, noise_f, wide, eip, elites, arrived, sums, parts, w1, w2, act, states, energy,
    asum, perm,
    load_sem, zs, zr, xs, xr, ns, nr, ss, sr,
):
    me = lax.axis_index("cand")
    z, x = me // NX, me % NX

    def zpeer(d):
        return {"cand": ((z + d) % NZ) * NX + x}

    def xpeer(j):
        return {"cand": z * NX + (x + j) % NX}

    def remote(src, dst, send, recv, peer):
        return pltpu.make_async_remote_copy(
            src_ref=src, dst_ref=dst, send_sem=send, recv_sem=recv,
            device_id=peer, device_id_type=pl.DeviceIdType.MESH,
        )

    barrier = pltpu.get_barrier_semaphore()
    for d in DIRECT[::-1]:
        pl.semaphore_signal(barrier, inc=1, device_id=zpeer(d), device_id_type=pl.DeviceIdType.MESH)
    for j in range(1, NX):
        pl.semaphore_signal(barrier, inc=1, device_id=xpeer(j), device_id_type=pl.DeviceIdType.MESH)

    small = [
        pltpu.make_async_copy(src, dst, load_sem.at[37 + i])
        for i, (src, dst) in enumerate(
            ((mean_hbm, mean_ref), (var_hbm, var_ref), (start_hbm, start_ref),
             (bias_hbm, bias_ref), (elite_hbm, elite_ref))
        )
    ]
    for c in small:
        c.start()
    loads = [pltpu.make_async_copy(noise_hbm, noise_v, load_sem.at[0])]
    for m in range(M):
        loads.append(pltpu.make_async_copy(wo_hbm.at[m], w2.at[m], load_sem.at[1 + m]))
        for r in range(4):
            n = 5 + 8 * m + 2 * r
            loads.append(
                pltpu.make_async_copy(ws_hbm.at[m], w1.at[m, r, pl.ds(0, S), :], load_sem.at[n])
            )
            loads.append(
                pltpu.make_async_copy(
                    wa_hbm.at[m], w1.at[m, r, pl.ds(S + ADIM * r, ADIM), :], load_sem.at[n + 1]
                )
            )
    for c in loads:
        c.start()

    for c in small:
        c.wait()
    rows[x, z, :, 0:F] = mean_ref[...]
    rows[x, z, :, F : 2 * F] = jnp.sqrt(var_ref[...])
    rows[x, z, :, 2 * F : ROW] = start_ref[...]

    pl.semaphore_wait(barrier, len(DIRECT) + NX - 1)

    mine = rows.at[x, z]
    z_out = [remote(mine, mine, zs.at[d], zr.at[d], zpeer(d)) for d in DIRECT[::-1]]
    for c in z_out:
        c.start()
    x_out = []
    for j in range(1, NX):
        x_out.append(remote(mine, mine, xs.at[0, j], xr.at[0, j], xpeer(j)))
        x_out[-1].start()
    wide[...] = jnp.full((E, 128), -1, jnp.int32)
    wide[:, 0:ELITE] = elite_ref[...]
    for k in range(NX):
        eip[NZ * k : NZ * (k + 1), :] = wide[pl.ds(k, NZ, stride=NX), :]
    listed = eip[...]
    first = me * CD
    chosen = [
        jnp.sum(jnp.where(listed == first + c, 1.0, 0.0), axis=1, keepdims=True) for c in range(CD)
    ]
    ranks, total = [], jnp.zeros((E, 1), F32)
    for c in range(CD):
        ranks.append(total)
        total = total + chosen[c]

    loads[0].wait()
    for q in range(4):
        part = noise_v[:, :, 128 * q : 128 * (q + 1)]
        noise_f[q] = part.astype(F32).reshape(E * CD, 128)

    def drawn_by(k, c):
        at = pl.ds(k * CD + c, NZ, stride=NX * CD)
        return jnp.concatenate([noise_f[q, at, :] for q in range(4)], axis=1)

    for k in range(NX):
        for s in range(CAP):
            slot = jnp.zeros((NZ, F), F32)
            for c in range(s, CD):
                cut = slice(NZ * k, NZ * (k + 1))
                pick = jnp.where(ranks[c][cut] == float(s), chosen[c][cut], 0.0)
                slot = slot + pick * drawn_by(k, c)
            elites[k, s] = slot.astype(BF)

    n_out = []
    for j in range(1, NX):
        n_out.append(
            remote(elites.at[(x + j) % NX], arrived.at[j], ns.at[j], nr.at[j], xpeer(j))
        )
        n_out[-1].start()

    for m in range(M):
        b = bias_ref[m : m + 1, :]
        hi = b.astype(BF).astype(F32)
        mid = (b - hi).astype(BF).astype(F32)
        low = b - hi - mid
        at = lax.broadcasted_iota(jnp.int32, (ADIM, HID), 0)
        tile = jnp.where(at == 0, hi, jnp.where(at == 1, mid, jnp.where(at == 2, low, 0.0)))
        tile = tile.astype(BF)
        for r in range(4):
            for k in range(4):
                if k != r:
                    w1[m, r, S + ADIM * k : S + ADIM * (k + 1), :] = (
                        tile if k == (r + 1) % 4 else jnp.zeros((ADIM, HID), BF)
                    )

    for d in NEAR:
        got = rows.at[x, (z - d + NZ) % NZ]
        remote(got, got, zs.at[d], zr.at[d], zpeer(d)).wait_recv()
        if d <= REACH or NZ - REACH < d:
            onward = REACH if d <= REACH else NZ - REACH
            far = (d + onward) % NZ
            z_out.append(remote(got, got, zs.at[far], zr.at[far], zpeer(onward)))
            z_out[-1].start()
        for j in range(1, NX):
            x_out.append(remote(got, got, xs.at[d, j], xr.at[d, j], xpeer(j)))
            x_out[-1].start()

    own = rows[x].reshape(NZ, ROW)
    line_mean, line_std = own[:, 0:F], own[:, F : 2 * F]
    line_listed = eip[pl.ds(pl.multiple_of(x * NZ, NZ), NZ), :] // CD
    first_sum = jnp.zeros((NZ, F), F32)
    second_sum = jnp.zeros((NZ, F), F32)
    for j in range(NX):
        block = z * NX + (x - j + NX) % NX
        count = jnp.sum(jnp.where(line_listed == block, 1.0, 0.0), axis=1, keepdims=True)
        if j > 0:
            n_out[j - 1].wait_recv()
        for s in range(CAP):
            drawn = (elites[x, s] if j == 0 else arrived[j, s]).astype(F32)
            a = jnp.clip(line_mean + line_std * drawn, -1.0, 1.0).astype(BF).astype(F32)
            a = jnp.where(count > float(s), a, 0.0)
            first_sum = first_sum + a
            second_sum = second_sum + a * a
    for k in range(4):
        cut = slice(128 * k, 128 * (k + 1))
        sums[pl.ds(k, NZ, stride=8), :] = first_sum[:, cut]
        sums[pl.ds(4 + k, NZ, stride=8), :] = second_sum[:, cut]

    def sum_copy(d):
        return remote(
            sums.at[pl.ds(pl.multiple_of(((z + d) % NZ) * 8, 8), 8), :],
            parts.at[pl.ds(8 * d, 8), :],
            ss.at[d], sr.at[d], zpeer(d),
        )

    s_out = [sum_copy(d) for d in NEAR[::-1]]
    for c in s_out:
        c.start()

    for d in (0,) + NEAR:
        for j in range(1, NX):
            got = rows.at[(x - j + NX) % NX, (z - d + NZ) % NZ]
            remote(got, got, xs.at[d, j], xr.at[d, j], xpeer(j)).wait_recv()

    gathered = [rows[k].reshape(NZ, ROW) for k in range(NX)]
    full_mean = jnp.concatenate([g[:, 0:F] for g in gathered], axis=0)
    full_std = jnp.concatenate([g[:, F : 2 * F] for g in gathered], axis=0)
    full_start = jnp.concatenate([g[:, 2 * F : ROW] for g in gathered], axis=0)
    for c in range(CD):
        m, h = c % M, c // M
        drawn = jnp.concatenate(
            [drawn_by(k, c) for k in range(NX)], axis=0
        )
        a = jnp.clip(full_mean + full_std * drawn, -1.0, 1.0).astype(BF).astype(F32)
        half = (0.5 * a).astype(BF)
        for q in range(4):
            act[m, q, E * h : E * (h + 1), :] = half[:, 128 * q : 128 * (q + 1)]
        asum[m, E * h : E * (h + 1), :] = jnp.sum(a * a, axis=1, keepdims=True)
        states[m, E * h : E * (h + 1), :] = full_start

    for c in loads[1:]:
        c.wait()
    lane = lax.broadcasted_iota(jnp.int32, (2 * E, 128), 1)

    def squares(s):
        return jnp.sum(s * s, axis=1, keepdims=True)

    def step(q, r):
        left = []
        for m in range(M):
            s = states[m]
            e = squares(s)
            energy[m] = energy[m] + e
            n = (s * (0.5 * lax.rsqrt(e * (1.0 / S) + EPSILON))).astype(BF)
            at = ADIM * ((r + 1) % 4)
            ones = jnp.where((lane >= at) & (lane < at + 3), 0.5, 0.0).astype(BF)
            now = (lane >= ADIM * r) & (lane < ADIM * (r + 1))
            left.append((s, jnp.concatenate([n, jnp.where(now, act[m, q], ones)], axis=1)))
        halves = [
            jnp.dot(left[m][1], w1[m, r], preferred_element_type=F32) for m in range(M)
        ]
        for m in range(M):
            h = halves[m]
            hidden = (h + h * jnp.tanh(h)).astype(BF)
            states[m] = left[m][0] + jnp.dot(hidden, w2[m], preferred_element_type=F32)

    initial = squares(full_start)
    for m in range(M):
        energy[m] = -jnp.concatenate([initial, initial], axis=0)

    def quarter(q, carry):
        for r in range(4):
            step(q, r)
        return carry

    lax.fori_loop(0, 4, quarter, 0)

    out_lane = lax.broadcasted_iota(jnp.int32, (E, 128), 1)
    table = jnp.zeros((E, 128), F32)
    for c in range(CD):
        m, h = c % M, c // M
        cut = slice(E * h, E * (h + 1))
        e = energy[m, cut, :] + squares(states[m, cut, :])
        value = e * (-1.0 / (S * HOR)) - asum[m, cut, :] * (0.1 / (ADIM * HOR))
        table = jnp.where(out_lane == c, value, table)
    for k in range(NX):
        perm[pl.ds(k, NZ, stride=NX), :] = table[NZ * k : NZ * (k + 1), :]
    ret_ref[...] = perm[...].T[0:CD, 0:E]

    total = sums[pl.ds(pl.multiple_of(z * 8, 8), 8), :]
    for d in NEAR:
        sum_copy(d).wait_recv()
        total = total + parts[8 * d : 8 * (d + 1), :]
    for k in range(4):
        cut = slice(128 * k, 128 * (k + 1))
        elite_mean = total[k : k + 1, :] * (1.0 / ELITE)
        elite_var = total[4 + k : 5 + k, :] * (1.0 / ELITE) - elite_mean * elite_mean
        nm_ref[:, cut] = ALPHA * mean_ref[:, cut] + (1.0 - ALPHA) * elite_mean
        nv_ref[:, cut] = ALPHA * var_ref[:, cut] + (1.0 - ALPHA) * elite_var

    for c in z_out + x_out + n_out + s_out:
        c.wait_send()


def put_out(a, b, c, a_out, b_out, c_out, a_v, b_v, c_v, sem):
    trips = ((a, a_v, a_out), (b, b_v, b_out), (c, c_v, c_out))
    taken = [pltpu.make_async_copy(src, mid, sem.at[i]) for i, (src, mid, _) in enumerate(trips)]
    given = [pltpu.make_async_copy(mid, dst, sem.at[i]) for i, (_, mid, dst) in enumerate(trips)]
    for copy in taken:
        copy.start()
    for i in range(3):
        taken[i].wait()
        given[i].start()
    for copy in given:
        copy.wait()


def per_device(mean, var, start, noise, elite, w_state, w_act, bias, w_out):
    vmem = pl.BlockSpec(memory_space=pltpu.VMEM)
    hbm = pl.BlockSpec(memory_space=pl.ANY)
    dma = pltpu.SemaphoreType.DMA
    shapes = (
            jax.ShapeDtypeStruct((CD, E), F32),
            jax.ShapeDtypeStruct((1, F), F32),
            jax.ShapeDtypeStruct((1, F), F32),
        )
    results = pl.pallas_call(
        kernel,
        out_shape=shapes,
        in_specs=[hbm] * 9,
        out_specs=(vmem, vmem, vmem),
        scratch_shapes=[
            pltpu.VMEM((1, F), F32),
            pltpu.VMEM((1, F), F32),
            pltpu.VMEM((1, S), F32),
            pltpu.VMEM((E, ELITE), jnp.int32),
            pltpu.VMEM((M, HID), F32),
            pltpu.VMEM((NX, NZ, 1, ROW), F32),
            pltpu.VMEM((E, CD, F), BF),
            pltpu.VMEM((4, E * CD, 128), F32),
            pltpu.VMEM((E, 128), jnp.int32),
            pltpu.VMEM((E, 128), jnp.int32),
            pltpu.VMEM((NX, CAP, NZ, F), BF),
            pltpu.VMEM((NX, CAP, NZ, F), BF),
            pltpu.VMEM((NZ * 8, 128), F32),
            pltpu.VMEM((NZ * 8, 128), F32),
            pltpu.VMEM((M, 4, 2 * S, HID), BF),
            pltpu.VMEM((M, HID, S), BF),
            pltpu.VMEM((M, 4, 2 * E, 128), BF),
            pltpu.VMEM((M, 2 * E, S), F32),
            pltpu.VMEM((M, 2 * E, 1), F32),
            pltpu.VMEM((M, 2 * E, 1), F32),
            pltpu.VMEM((128, 128), F32),
            dma((42,)), dma((NZ,)), dma((NZ,)), dma((NZ, NX)), dma((NZ, NX)),
            dma((NX,)), dma((NX,)), dma((NZ,)), dma((NZ,)),
        ],
        compiler_params=pltpu.CompilerParams(
            collective_id=0, has_side_effects=True, vmem_limit_bytes=60 * 1024 * 2**10
        ),
    )(mean, var, start, noise, elite, w_state, w_act, bias, w_out)
    returns, new_mean, new_var = pl.pallas_call(
        put_out,
        out_shape=shapes,
        in_specs=[hbm] * 3,
        out_specs=(hbm, hbm, hbm),
        scratch_shapes=[pltpu.VMEM(s.shape, s.dtype) for s in shapes] + [dma((3,))],
        compiler_params=pltpu.CompilerParams(vmem_limit_bytes=60 * 1024 * 2**10),
    )(*results)
    return returns.T, new_mean, new_var


def solution(mesh):
    both = P(("env", "cand"), None)
    in_specs = (both, both, both, P("env", "cand", None), P("env", None), P(), P(), P(), P())
    return jax.shard_map(
        per_device, mesh=mesh, in_specs=in_specs, out_specs=(P("env", "cand"), both, both),
        check_vma=False,
    )
```

```python
import functools

import jax
import jax.numpy as jnp
from jax import lax
from jax.experimental import pallas as pl
from jax.experimental.pallas import tpu as pltpu
from jax.sharding import PartitionSpec as P

BF = jnp.bfloat16
F32 = jnp.float32
ALPHA = 0.1
EPSILON = 1e-06
NX, NZ = 4, 16
ELITE, CAP, CD = 64, 4, 8
S, ADIM, HID, F, M, HOR = 128, 32, 512, 512, 4, 16
E = NX * NZ
ROW = 2 * F + S
REACH = 4
DIRECT = (1, 15, 2, 14, 3, 13, 4, 12)
RELAYED = (5, 11, 6, 10, 7, 9, 8)
NEAR = DIRECT + RELAYED


def kernel(
    mean_hbm, var_hbm, start_hbm, noise_hbm, elite_hbm, ws_hbm, wa_hbm, bias_hbm, wo_hbm,
    ret_ref, nm_ref, nv_ref,
    mean_ref, var_ref, start_ref, elite_ref, bias_ref, rows, noise_v, noise_f, wide, eip, elites, arrived, sums, parts, w1, w2, act, states, energy,
    asum, perm,
    load_sem, zs, zr, xs, xr, ns, nr, ss, sr,
):
    me = lax.axis_index("cand")
    z, x = lax.div(me, NX), lax.rem(me, NX)

    def zpeer(d):
        return {"cand": lax.rem(me + NX * d, E)}

    def xpeer(j):
        return {"cand": z * NX + lax.rem(x + j, NX)}

    def zback(d):
        return lax.rem(z + NZ - d, NZ)

    def xback(j):
        return lax.rem(x + NX - j, NX)

    def remote(src, dst, send, recv, peer):
        return pltpu.make_async_remote_copy(
            src_ref=src, dst_ref=dst, send_sem=send, recv_sem=recv,
            device_id=peer, device_id_type=pl.DeviceIdType.MESH,
        )

    small = [
        pltpu.make_async_copy(src, dst, load_sem.at[i])
        for i, (src, dst) in enumerate(
            ((mean_hbm, mean_ref), (var_hbm, var_ref), (start_hbm, start_ref),
             (bias_hbm, bias_ref), (elite_hbm, elite_ref), (noise_hbm, noise_v))
        )
    ]
    for c in small[:3]:
        c.start()
    barrier = pltpu.get_barrier_semaphore()
    for d in DIRECT[::-1]:
        pl.semaphore_signal(barrier, inc=1, device_id=zpeer(d), device_id_type=pl.DeviceIdType.MESH)
    for j in range(1, NX):
        pl.semaphore_signal(barrier, inc=1, device_id=xpeer(j), device_id_type=pl.DeviceIdType.MESH)
    for c in small[3:]:
        c.start()

    for c in small[:3]:
        c.wait()
    rows[x, z, :, 0:F] = mean_ref[...]
    rows[x, z, :, F : 2 * F] = jnp.sqrt(var_ref[...])
    rows[x, z, :, 2 * F : ROW] = start_ref[...]

    pl.semaphore_wait(barrier, len(DIRECT) + NX - 1)

    mine = rows.at[x, z]
    for d in DIRECT[::-1]:
        remote(mine, mine, zs, zr.at[d], zpeer(d)).start()
    for j in range(1, NX):
        remote(mine, mine, xs, xr.at[j], xpeer(j)).start()

    for m in range(M):
        pltpu.make_async_copy(wo_hbm.at[m], w2.at[m], load_sem.at[6]).start()
        for r in range(4):
            pltpu.make_async_copy(ws_hbm.at[m], w1.at[m, r, 0:S, :], load_sem.at[7]).start()
            rest = w1.at[m, r, S + ADIM * r : S + ADIM * (r + 1), :]
            pltpu.make_async_copy(wa_hbm.at[m], rest, load_sem.at[7]).start()

    small[4].wait()
    wide[...] = jnp.full((E, 128), -1, jnp.int32)
    wide[:, 0:ELITE] = elite_ref[...]
    for k in range(NX):
        eip[NZ * k : NZ * (k + 1), :] = wide[pl.ds(k, NZ, stride=NX), :]

    small[5].wait()
    for q in range(4):
        part = noise_v[:, :, 128 * q : 128 * (q + 1)]
        noise_f[q] = part.astype(F32).reshape(E * CD, 128)

    def drawn_by(k, c):
        at = pl.ds(k * CD + c, NZ, stride=NX * CD)
        return jnp.concatenate([noise_f[q, at, :] for q in range(4)], axis=1)

    for k in range(NX):
        listed = eip[NZ * k : NZ * (k + 1), :]
        before = jnp.zeros((NZ, 1), F32)
        slots = [jnp.zeros((NZ, F), F32) for _ in range(CAP)]
        for c in range(CD):
            hit = jnp.where(listed == me * CD + c, 1.0, 0.0)
            chosen = jnp.sum(hit, axis=1, keepdims=True)
            drawn = drawn_by(k, c)
            place = jnp.where(chosen > 0.5, before, -1.0)
            for s in range(min(c + 1, CAP)):
                slots[s] = jnp.where(place == float(s), drawn, slots[s])
            before = before + chosen
        for s in range(CAP):
            elites[k, s] = slots[s].astype(BF)

    for j in range(1, NX):
        remote(elites.at[lax.rem(x + j, NX)], arrived.at[j], ns, nr.at[j], xpeer(j)).start()

    small[3].wait()
    for m in range(M):
        b = bias_ref[m : m + 1, :]
        hi = b.astype(BF).astype(F32)
        mid = (b - hi).astype(BF).astype(F32)
        low = b - hi - mid
        at = lax.broadcasted_iota(jnp.int32, (ADIM, HID), 0)
        tile = jnp.where(at == 0, hi, jnp.where(at == 1, mid, jnp.where(at == 2, low, 0.0)))
        tile = tile.astype(BF)
        for r in range(4):
            for k in range(4):
                if k != r:
                    w1[m, r, S + ADIM * k : S + ADIM * (k + 1), :] = (
                        tile if k == (r + 1) % 4 else jnp.zeros((ADIM, HID), BF)
                    )

    for d in NEAR:
        got = rows.at[x, zback(d)]
        remote(got, got, zs, zr.at[d], zpeer(d)).wait_recv()
        if d <= REACH or NZ - REACH < d:
            onward = REACH if d <= REACH else NZ - REACH
            remote(got, got, zs, zr.at[(d + onward) % NZ], zpeer(onward)).start()
        for j in range(1, NX):
            remote(got, got, xs, xr.at[j], xpeer(j)).start()

    own = rows[x].reshape(NZ, ROW)
    line_mean, line_std = own[:, 0:F], own[:, F : 2 * F]
    line_listed = eip[pl.ds(pl.multiple_of(x * NZ, NZ), NZ), :] // CD
    first_sum = jnp.zeros((NZ, F), F32)
    second_sum = jnp.zeros((NZ, F), F32)
    for j in range(NX):
        block = z * NX + xback(j)
        count = jnp.sum(jnp.where(line_listed == block, 1.0, 0.0), axis=1, keepdims=True)
        if j > 0:
            remote(elites.at[0], arrived.at[j], ns, nr.at[j], xpeer(j)).wait_recv()
        for s in range(CAP):
            drawn = (elites[x, s] if j == 0 else arrived[j, s]).astype(F32)
            a = jnp.clip(line_mean + line_std * drawn, -1.0, 1.0).astype(BF).astype(F32)
            a = jnp.where(count > float(s), a, 0.0)
            first_sum = first_sum + a
            second_sum = second_sum + a * a
    for k in range(4):
        cut = slice(128 * k, 128 * (k + 1))
        sums[pl.ds(k, NZ, stride=8), :] = first_sum[:, cut]
        sums[pl.ds(4 + k, NZ, stride=8), :] = second_sum[:, cut]

    for d in NEAR[::-1]:
        remote(
            sums.at[pl.ds(pl.multiple_of(lax.rem(z + d, NZ) * 8, 8), 8), :],
            parts.at[pl.ds(8 * d, 8), :],
            ss, sr, zpeer(d),
        ).start()

    for j in range(NX):
        k = xback(j)
        if j > 0:
            remote(rows.at[k], rows.at[k], xs, xr.at[j], xpeer(j)).wait_recv()
        line = rows[k].reshape(NZ, ROW)
        line_mean, line_std = line[:, 0:F], line[:, F : 2 * F]
        line_start = line[:, 2 * F : ROW]
        initial = -jnp.sum(line_start * line_start, axis=1, keepdims=True)
        for c in range(CD):
            m, h = c % M, c // M
            cut = slice(E * h + NZ * j, E * h + NZ * (j + 1))
            a = jnp.clip(line_mean + line_std * drawn_by(k, c), -1.0, 1.0).astype(BF)
            half = a * jnp.asarray(0.5, BF)
            for q in range(4):
                act[m, q, cut, :] = half[:, 128 * q : 128 * (q + 1)]
            a = a.astype(F32)
            asum[m, cut, :] = jnp.sum(a * a, axis=1, keepdims=True)
            states[m, cut, :] = line_start
            energy[m, cut, :] = initial

    pltpu.make_async_copy(wo_hbm, w2, load_sem.at[6]).wait()
    filled = w1.at[:, :, 0 : S + ADIM, :]
    pltpu.make_async_copy(filled, filled, load_sem.at[7]).wait()
    lane = lax.broadcasted_iota(jnp.int32, (2 * E, 128), 1)

    def squares(s):
        return jnp.sum(s * s, axis=1, keepdims=True)

    def step(q, r):
        left = []
        for m in range(M):
            s = states[m]
            e = squares(s)
            energy[m] = energy[m] + e
            n = (s * (0.5 * lax.rsqrt(e * (1.0 / S) + EPSILON))).astype(BF)
            at = ADIM * ((r + 1) % 4)
            ones = jnp.where((lane >= at) & (lane < at + 3), 0.5, 0.0).astype(BF)
            now = (lane >= ADIM * r) & (lane < ADIM * (r + 1))
            left.append((s, jnp.concatenate([n, jnp.where(now, act[m, q], ones)], axis=1)))
        halves = [
            jnp.dot(left[m][1], w1[m, r], preferred_element_type=F32) for m in range(M)
        ]
        for m in range(M):
            h = halves[m]
            hidden = (h + h * jnp.tanh(h)).astype(BF)
            states[m] = left[m][0] + jnp.dot(hidden, w2[m], preferred_element_type=F32)

    def quarter(q, carry):
        for r in range(4):
            step(q, r)
        return carry

    lax.fori_loop(0, 4, quarter, 0)

    out_lane = lax.broadcasted_iota(jnp.int32, (E, 128), 1)
    table = jnp.zeros((E, 128), F32)
    for c in range(CD):
        m, h = c % M, c // M
        cut = slice(E * h, E * (h + 1))
        e = energy[m, cut, :] + squares(states[m, cut, :])
        value = e * (-1.0 / (S * HOR)) - asum[m, cut, :] * (0.1 / (ADIM * HOR))
        table = jnp.where(out_lane == c, value, table)
    for j in range(NX):
        perm[pl.ds(xback(j), NZ, stride=NX), :] = table[NZ * j : NZ * (j + 1), :]
    ret_ref[...] = perm[...].T[0:CD, 0:E]

    others = parts.at[pl.ds(8, 8 * (NZ - 1)), :]
    remote(others, others, ss, sr, zpeer(1)).wait_recv()
    total = sums[pl.ds(pl.multiple_of(z * 8, 8), 8), :]
    for d in range(1, NZ):
        total = total + parts[8 * d : 8 * (d + 1), :]
    for k in range(4):
        cut = slice(128 * k, 128 * (k + 1))
        elite_mean = total[k : k + 1, :] * (1.0 / ELITE)
        elite_var = total[4 + k : 5 + k, :] * (1.0 / ELITE) - elite_mean * elite_mean
        nm_ref[:, cut] = ALPHA * mean_ref[:, cut] + (1.0 - ALPHA) * elite_mean
        nv_ref[:, cut] = ALPHA * var_ref[:, cut] + (1.0 - ALPHA) * elite_var

    remote(others, others, ss, sr, zpeer(1)).wait_send()
    sent = rows.at[0, pl.ds(0, NZ - 1)]
    remote(sent, sent, zs, zr.at[1], zpeer(1)).wait_send()
    sent = rows.at[pl.ds(0, NX - 1)]
    remote(sent, sent, xs, xr.at[1], xpeer(1)).wait_send()
    sent = arrived.at[pl.ds(1, NX - 1)]
    remote(sent, sent, ns, nr.at[1], xpeer(1)).wait_send()


def put_out(a, b, c, a_out, b_out, c_out, sem):
    copies = [
        pltpu.make_async_copy(src, dst, sem.at[i])
        for i, (src, dst) in enumerate(((a, a_out), (b, b_out), (c, c_out)))
    ]
    for copy in copies:
        copy.start()
    for copy in copies:
        copy.wait()


def per_device(*operands):
    vmem = pl.BlockSpec(memory_space=pltpu.VMEM)
    hbm = pl.BlockSpec(memory_space=pl.ANY)
    dma = pltpu.SemaphoreType.DMA
    shapes = (
            jax.ShapeDtypeStruct((CD, E), F32),
            jax.ShapeDtypeStruct((1, F), F32),
            jax.ShapeDtypeStruct((1, F), F32),
        )
    results = pl.pallas_call(
        kernel,
        out_shape=shapes,
        in_specs=[hbm] * 9,
        out_specs=(vmem, vmem, vmem),
        scratch_shapes=[
            pltpu.VMEM((1, F), F32),
            pltpu.VMEM((1, F), F32),
            pltpu.VMEM((1, S), F32),
            pltpu.VMEM((E, ELITE), jnp.int32),
            pltpu.VMEM((M, HID), F32),
            pltpu.VMEM((NX, NZ, 1, ROW), F32),
            pltpu.VMEM((E, CD, F), BF),
            pltpu.VMEM((4, E * CD, 128), F32),
            pltpu.VMEM((E, 128), jnp.int32),
            pltpu.VMEM((E, 128), jnp.int32),
            pltpu.VMEM((NX, CAP, NZ, F), BF),
            pltpu.VMEM((NX, CAP, NZ, F), BF),
            pltpu.VMEM((NZ * 8, 128), F32),
            pltpu.VMEM((NZ * 8, 128), F32),
            pltpu.VMEM((M, 4, 2 * S, HID), BF),
            pltpu.VMEM((M, HID, S), BF),
            pltpu.VMEM((M, 4, 2 * E, 128), BF),
            pltpu.VMEM((M, 2 * E, S), F32),
            pltpu.VMEM((M, 2 * E, 1), F32),
            pltpu.VMEM((M, 2 * E, 1), F32),
            pltpu.VMEM((128, 128), F32),
            dma((8,)), dma, dma((NZ,)), dma, dma((NX,)), dma, dma((NX,)), dma, dma,
        ],
        compiler_params=pltpu.CompilerParams(
            collective_id=0, has_side_effects=True, vmem_limit_bytes=24 * 2**20
        ),
    )(*(pltpu.with_memory_space_constraint(a, pltpu.HBM) for a in operands))
    returns, new_mean, new_var = pl.pallas_call(
        put_out,
        out_shape=shapes,
        in_specs=[vmem] * 3,
        out_specs=(hbm, hbm, hbm),
        scratch_shapes=[dma((3,))],
        compiler_params=pltpu.CompilerParams(vmem_limit_bytes=24 * 2**20),
    )(*results)
    return returns.T, new_mean, new_var


def solution(mesh):
    both = P(("env", "cand"), None)
    in_specs = (both, both, both, P("env", "cand", None), P("env", None), P(), P(), P(), P())
    return jax.shard_map(
        per_device, mesh=mesh, in_specs=in_specs, out_specs=(P("env", "cand"), both, both),
        check_vma=False,
    )
```

```python
import functools

import jax
import jax.numpy as jnp
from jax import lax
from jax.experimental import pallas as pl
from jax.experimental.pallas import tpu as pltpu
from jax.sharding import PartitionSpec as P

BF = jnp.bfloat16
F32 = jnp.float32
ALPHA = 0.1
EPSILON = 1e-06
NX, NZ = 4, 16
ELITE, CAP, CD = 64, 4, 8
S, ADIM, HID, F, M, HOR = 128, 32, 512, 512, 4, 16
E = NX * NZ
ROW = 2 * F + S
REACH = 4
DIRECT = (1, 15, 2, 14, 3, 13, 4, 12)
RELAYED = (5, 11, 6, 10, 7, 9, 8)
NEAR = DIRECT + RELAYED


def kernel(
    mean_hbm, var_hbm, start_hbm, noise_hbm, elite_hbm, ws_hbm, wa_hbm, bias_hbm, wo_hbm,
    ret_ref, nm_ref, nv_ref,
    mean_ref, var_ref, start_ref, elite_ref, bias_ref, rows, guests, noise_v, noise_f, noise_c, wide, eip, elites, arrived, sums, parts, w1, w2, act, states, energy,
    asum, perm,
    load_sem, gs, gr, zs, zr, xs, xr, ns, nr, ss, sr,
):
    me = lax.axis_index("cand")
    z, x = lax.div(me, NX), lax.rem(me, NX)

    env = lax.axis_index("env")
    core = lax.rem(env, 2)
    relays_two, is_guest = core == 1, core == 0

    def zpeer(d, over=0):
        return {"cand": lax.rem(me + NX * d, E), "env": env + over}

    def xpeer(j, over=0):
        return {"cand": z * NX + lax.rem(x + j, NX), "env": env + over}

    def zback(d):
        return lax.rem(z + NZ - d, NZ)

    def xback(j):
        return lax.rem(x + NX - j, NX)

    def remote(src, dst, send, recv, peer):
        return pltpu.make_async_remote_copy(
            src_ref=src, dst_ref=dst, send_sem=send, recv_sem=recv,
            device_id=peer, device_id_type=pl.DeviceIdType.MESH,
        )

    small = [
        pltpu.make_async_copy(src, dst, load_sem.at[i])
        for i, (src, dst) in enumerate(
            ((mean_hbm, mean_ref), (var_hbm, var_ref), (start_hbm, start_ref),
             (bias_hbm, bias_ref), (elite_hbm, elite_ref), (noise_hbm, noise_v))
        )
    ]
    for c in small[:3]:
        c.start()
    barrier = pltpu.get_barrier_semaphore()

    def greet(peer):
        pl.semaphore_signal(barrier, inc=1, device_id=peer, device_id_type=pl.DeviceIdType.MESH)

    @pl.when(relays_two)
    def _():
        for d in DIRECT[::-1]:
            greet(zpeer(d, -1))
            greet(zpeer(d))

    @pl.when(is_guest)
    def _():
        for j in range(NX):
            greet(xpeer(j, 1))

    for j in range(1, NX):
        greet(xpeer(j))
    for c in small[3:]:
        c.start()

    for c in small[:3]:
        c.wait()
    rows[x, z, :, 0:F] = mean_ref[...]
    rows[x, z, :, F : 2 * F] = jnp.sqrt(var_ref[...])
    rows[x, z, :, 2 * F : ROW] = start_ref[...]

    pl.semaphore_wait(barrier, len(DIRECT) + NX - 1 + NX * core)

    mine = rows.at[x, z]

    @pl.when(relays_two)
    def _():
        for d in DIRECT[::-1]:
            remote(mine, mine, zs, zr.at[d], zpeer(d)).start()

    @pl.when(is_guest)
    def _():
        for d in DIRECT[::-1]:
            remote(mine, guests.at[z], zs, gr.at[d], zpeer(d, 1)).start()

    for j in range(1, NX):
        remote(mine, mine, xs, xr.at[j], xpeer(j)).start()

    for m in range(M):
        pltpu.make_async_copy(wo_hbm.at[m], w2.at[m], load_sem.at[6]).start()
        for r in range(4):
            pltpu.make_async_copy(ws_hbm.at[m], w1.at[m, r, 0:S, :], load_sem.at[7]).start()
            rest = w1.at[m, r, S + ADIM * r : S + ADIM * (r + 1), :]
            pltpu.make_async_copy(wa_hbm.at[m], rest, load_sem.at[7]).start()

    small[4].wait()
    wide[...] = jnp.full((E, 128), -1, jnp.int32)
    wide[:, 0:ELITE] = elite_ref[...]
    for k in range(NX):
        eip[NZ * k : NZ * (k + 1), :] = wide[pl.ds(k, NZ, stride=NX), :]

    small[5].wait()
    for q in range(4):
        part = noise_v[:, :, 128 * q : 128 * (q + 1)]
        noise_f[q] = part.astype(F32).reshape(E * CD, 128)

    for k in range(NX):
        listed = eip[NZ * k : NZ * (k + 1), :]
        before = jnp.zeros((NZ, 1), F32)
        slots = [jnp.zeros((NZ, F), F32) for _ in range(CAP)]
        for c in range(CD):
            hit = jnp.where(listed == me * CD + c, 1.0, 0.0)
            chosen = jnp.sum(hit, axis=1, keepdims=True)
            at = pl.ds(k * CD + c, NZ, stride=NX * CD)
            drawn = jnp.concatenate([noise_f[q, at, :] for q in range(4)], axis=1)
            noise_c[k, c] = drawn
            place = jnp.where(chosen > 0.5, before, -1.0)
            for s in range(min(c + 1, CAP)):
                slots[s] = jnp.where(place == float(s), drawn, slots[s])
            before = before + chosen
        for s in range(CAP):
            elites[k, s] = slots[s].astype(BF)

    for j in range(1, NX):
        remote(elites.at[lax.rem(x + j, NX)], arrived.at[j], ns, nr.at[j], xpeer(j)).start()

    small[3].wait()
    for m in range(M):
        b = bias_ref[m : m + 1, :]
        hi = b.astype(BF).astype(F32)
        mid = (b - hi).astype(BF).astype(F32)
        low = b - hi - mid
        at = lax.broadcasted_iota(jnp.int32, (ADIM, HID), 0)
        tile = jnp.where(at == 0, hi, jnp.where(at == 1, mid, jnp.where(at == 2, low, 0.0)))
        tile = tile.astype(BF)
        for r in range(4):
            for k in range(4):
                if k != r:
                    w1[m, r, S + ADIM * k : S + ADIM * (k + 1), :] = (
                        tile if k == (r + 1) % 4 else jnp.zeros((ADIM, HID), BF)
                    )

    @pl.when(relays_two)
    def _():
        for d in NEAR:
            near = d <= REACH or NZ - REACH < d
            onward = REACH if d <= REACH else NZ - REACH
            far = (d + onward) % NZ
            guest, seat = guests.at[zback(d)], rows.at[x, zback(d)]
            remote(guest, guest, gs.at[1], gr.at[d], zpeer(d)).wait_recv()
            if near:
                remote(guest, guest, gs.at[1], gr.at[far], zpeer(onward)).start()
            for j in (2, 1, 3):
                remote(guest, seat, gs.at[0], xr.at[j], xpeer(j, -1)).start()
            remote(guest, seat, gs.at[1], zr.at[d], xpeer(0, -1)).start()
            remote(seat, seat, zs, zr.at[d], zpeer(d)).wait_recv()
            if near:
                remote(seat, seat, zs, zr.at[far], zpeer(onward)).start()
            for j in (2, 1, 3):
                remote(seat, seat, xs, xr.at[j], xpeer(j)).start()

    @pl.when(is_guest)
    def _():
        for d in NEAR:
            seat = rows.at[x, zback(d)]
            remote(seat, seat, zs, zr.at[d], zpeer(d)).wait_recv()

    own = rows[x].reshape(NZ, ROW)
    line_mean, line_std = own[:, 0:F], own[:, F : 2 * F]
    line_listed = eip[pl.ds(pl.multiple_of(x * NZ, NZ), NZ), :] // CD
    first_sum = jnp.zeros((NZ, F), F32)
    second_sum = jnp.zeros((NZ, F), F32)
    for j in range(NX):
        block = z * NX + xback(j)
        count = jnp.sum(jnp.where(line_listed == block, 1.0, 0.0), axis=1, keepdims=True)
        if j > 0:
            remote(elites.at[0], arrived.at[j], ns, nr.at[j], xpeer(j)).wait_recv()
        for s in range(CAP):
            drawn = (elites[x, s] if j == 0 else arrived[j, s]).astype(F32)
            a = jnp.clip(line_mean + line_std * drawn, -1.0, 1.0).astype(BF).astype(F32)
            a = jnp.where(count > float(s), a, 0.0)
            first_sum = first_sum + a
            second_sum = second_sum + a * a
    for k in range(4):
        cut = slice(128 * k, 128 * (k + 1))
        sums[pl.ds(k, NZ, stride=8), :] = first_sum[:, cut]
        sums[pl.ds(4 + k, NZ, stride=8), :] = second_sum[:, cut]

    for d in NEAR[::-1]:
        remote(
            sums.at[pl.ds(pl.multiple_of(lax.rem(z + d, NZ) * 8, 8), 8), :],
            parts.at[pl.ds(8 * d, 8), :],
            ss, sr, zpeer(d),
        ).start()

    for j in range(NX):
        k = xback(j)
        if j > 0:
            remote(rows.at[k], rows.at[k], xs, xr.at[j], xpeer(j)).wait_recv()
        line = rows[k].reshape(NZ, ROW)
        line_mean, line_std = line[:, 0:F], line[:, F : 2 * F]
        line_start = line[:, 2 * F : ROW]
        initial = -jnp.sum(line_start * line_start, axis=1, keepdims=True)
        for c in range(CD):
            m, h = c % M, c // M
            cut = slice(E * h + NZ * j, E * h + NZ * (j + 1))
            a = jnp.clip(line_mean + line_std * noise_c[k, c], -1.0, 1.0).astype(BF)
            half = a * jnp.asarray(0.5, BF)
            for q in range(4):
                act[m, q, cut, :] = half[:, 128 * q : 128 * (q + 1)]
            a = a.astype(F32)
            asum[m, cut, :] = jnp.sum(a * a, axis=1, keepdims=True)
            states[m, cut, :] = line_start
            energy[m, cut, :] = initial

    pltpu.make_async_copy(wo_hbm, w2, load_sem.at[6]).wait()
    filled = w1.at[:, :, 0 : S + ADIM, :]
    pltpu.make_async_copy(filled, filled, load_sem.at[7]).wait()
    lane = lax.broadcasted_iota(jnp.int32, (2 * E, 128), 1)

    def squares(s):
        return jnp.sum(s * s, axis=1, keepdims=True)

    def step(q, r):
        left = []
        for m in range(M):
            s = states[m]
            e = squares(s)
            energy[m] = energy[m] + e
            n = (s * (0.5 * lax.rsqrt(e * (1.0 / S) + EPSILON))).astype(BF)
            at = ADIM * ((r + 1) % 4)
            ones = jnp.where((lane >= at) & (lane < at + 3), 0.5, 0.0).astype(BF)
            now = (lane >= ADIM * r) & (lane < ADIM * (r + 1))
            left.append((s, jnp.concatenate([n, jnp.where(now, act[m, q], ones)], axis=1)))
        halves = [
            jnp.dot(left[m][1], w1[m, r], preferred_element_type=F32) for m in range(M)
        ]
        for m in range(M):
            h = halves[m]
            hidden = (h + h * jnp.tanh(h)).astype(BF)
            states[m] = left[m][0] + jnp.dot(hidden, w2[m], preferred_element_type=F32)

    def quarter(q, carry):
        for r in range(4):
            step(q, r)
        return carry

    lax.fori_loop(0, 4, quarter, 0)

    out_lane = lax.broadcasted_iota(jnp.int32, (E, 128), 1)
    table = jnp.zeros((E, 128), F32)
    for c in range(CD):
        m, h = c % M, c // M
        cut = slice(E * h, E * (h + 1))
        e = energy[m, cut, :] + squares(states[m, cut, :])
        value = e * (-1.0 / (S * HOR)) - asum[m, cut, :] * (0.1 / (ADIM * HOR))
        table = jnp.where(out_lane == c, value, table)
    for j in range(NX):
        perm[pl.ds(xback(j), NZ, stride=NX), :] = table[NZ * j : NZ * (j + 1), :]
    ret_ref[...] = perm[...].T[0:CD, 0:E]

    others = parts.at[pl.ds(8, 8 * (NZ - 1)), :]
    remote(others, others, ss, sr, zpeer(1)).wait_recv()
    total = sums[pl.ds(pl.multiple_of(z * 8, 8), 8), :]
    for d in range(1, NZ):
        total = total + parts[8 * d : 8 * (d + 1), :]
    for k in range(4):
        cut = slice(128 * k, 128 * (k + 1))
        elite_mean = total[k : k + 1, :] * (1.0 / ELITE)
        elite_var = total[4 + k : 5 + k, :] * (1.0 / ELITE) - elite_mean * elite_mean
        nm_ref[:, cut] = ALPHA * mean_ref[:, cut] + (1.0 - ALPHA) * elite_mean
        nv_ref[:, cut] = ALPHA * var_ref[:, cut] + (1.0 - ALPHA) * elite_var

    remote(others, others, ss, sr, zpeer(1)).wait_send()

    @pl.when(relays_two)
    def _():
        near_and_far = rows.at[0, pl.ds(0, NZ - 1)]
        remote(near_and_far, near_and_far, zs, zr.at[1], zpeer(1)).wait_send()
        sideways = rows.at[pl.ds(0, NX - 1)]
        remote(sideways, sideways, xs, xr.at[1], xpeer(1)).wait_send()
        guests_sideways = rows.at[pl.ds(0, NX - 1), pl.ds(0, NZ - 1)]
        remote(guests_sideways, guests_sideways, gs.at[0], xr.at[1], xpeer(1)).wait_send()
        guests_other = rows.at[pl.ds(0, 2), pl.ds(0, (2 * NZ + REACH * 2 - 2 - NZ) // 2)]
        remote(guests_other, guests_other, gs.at[1], xr.at[1], xpeer(1)).wait_send()

    @pl.when(is_guest)
    def _():
        near = rows.at[0, pl.ds(0, len(DIRECT))]
        remote(near, near, zs, zr.at[1], zpeer(1)).wait_send()
        sideways = rows.at[0, pl.ds(0, NX - 1)]
        remote(sideways, sideways, xs, xr.at[1], xpeer(1)).wait_send()

    sent = arrived.at[pl.ds(1, NX - 1)]
    remote(sent, sent, ns, nr.at[1], xpeer(1)).wait_send()


def put_out(a, b, c, a_out, b_out, c_out, sem):
    copies = [
        pltpu.make_async_copy(src, dst, sem.at[i])
        for i, (src, dst) in enumerate(((a, a_out), (b, b_out), (c, c_out)))
    ]
    for copy in copies:
        copy.start()
    for copy in copies:
        copy.wait()


def per_device(*operands):
    vmem = pl.BlockSpec(memory_space=pltpu.VMEM)
    hbm = pl.BlockSpec(memory_space=pl.ANY)
    dma = pltpu.SemaphoreType.DMA
    shapes = (
            jax.ShapeDtypeStruct((CD, E), F32),
            jax.ShapeDtypeStruct((1, F), F32),
            jax.ShapeDtypeStruct((1, F), F32),
        )
    results = pl.pallas_call(
        kernel,
        out_shape=shapes,
        in_specs=[hbm] * 9,
        out_specs=(vmem, vmem, vmem),
        scratch_shapes=[
            pltpu.VMEM((1, F), F32),
            pltpu.VMEM((1, F), F32),
            pltpu.VMEM((1, S), F32),
            pltpu.VMEM((E, ELITE), jnp.int32),
            pltpu.VMEM((M, HID), F32),
            pltpu.VMEM((NX, NZ, 1, ROW), F32),
            pltpu.VMEM((NZ, 1, ROW), F32),
            pltpu.VMEM((E, CD, F), BF),
            pltpu.VMEM((4, E * CD, 128), F32),
            pltpu.VMEM((NX, CD, NZ, F), F32),
            pltpu.VMEM((E, 128), jnp.int32),
            pltpu.VMEM((E, 128), jnp.int32),
            pltpu.VMEM((NX, CAP, NZ, F), BF),
            pltpu.VMEM((NX, CAP, NZ, F), BF),
            pltpu.VMEM((NZ * 8, 128), F32),
            pltpu.VMEM((NZ * 8, 128), F32),
            pltpu.VMEM((M, 4, 2 * S, HID), BF),
            pltpu.VMEM((M, HID, S), BF),
            pltpu.VMEM((M, 4, 2 * E, 128), BF),
            pltpu.VMEM((M, 2 * E, S), F32),
            pltpu.VMEM((M, 2 * E, 1), F32),
            pltpu.VMEM((M, 2 * E, 1), F32),
            pltpu.VMEM((128, 128), F32),
            dma((8,)), dma((2,)), dma((NZ,)), dma, dma((NZ,)), dma, dma((NX,)), dma, dma((NX,)), dma, dma,
        ],
        compiler_params=pltpu.CompilerParams(
            collective_id=0, has_side_effects=True, vmem_limit_bytes=24 * 2**20
        ),
    )(*(pltpu.with_memory_space_constraint(a, pltpu.HBM) for a in operands))
    returns, new_mean, new_var = pl.pallas_call(
        put_out,
        out_shape=shapes,
        in_specs=[vmem] * 3,
        out_specs=(hbm, hbm, hbm),
        scratch_shapes=[dma((3,))],
        compiler_params=pltpu.CompilerParams(vmem_limit_bytes=24 * 2**20),
    )(*results)
    return returns.T, new_mean, new_var


def solution(mesh):
    both = P(("env", "cand"), None)
    in_specs = (both, both, both, P("env", "cand", None), P("env", None), P(), P(), P(), P())
    return jax.shard_map(
        per_device, mesh=mesh, in_specs=in_specs, out_specs=(P("env", "cand"), both, both),
        check_vma=False,
    )
```

```python
import functools

import jax
import jax.numpy as jnp
from jax import lax
from jax.experimental import pallas as pl
from jax.experimental.pallas import tpu as pltpu
from jax.sharding import PartitionSpec as P

BF = jnp.bfloat16
F32 = jnp.float32
ALPHA = 0.1
EPSILON = 1e-06
NX, NZ = 4, 16
ELITE, CAP, CD = 64, 4, 8
S, ADIM, HID, F, M, HOR = 128, 32, 512, 512, 4, 16
E = NX * NZ
ROW = 2 * F + S
REACH = 4
DIRECT = (1, 15, 2, 14, 3, 13, 4, 12)
RELAYED = (5, 11, 6, 10, 7, 9, 8)
NEAR = DIRECT + RELAYED


def kernel(
    mean_hbm, var_hbm, start_hbm, noise_hbm, elite_hbm, ws_hbm, wa_hbm, bias_hbm, wo_hbm,
    ret_ref, nm_ref, nv_ref,
    mean_ref, var_ref, start_ref, elite_ref, bias_ref, rows, guests, noise_v, noise_f, noise_c, wide, eip, elites, arrived, sums, parts, w1, w2, act, states, energy,
    asum, perm,
    load_sem, gs, gr, zs, zr, xs, xr, ns, nr, ss, sr,
):
    me = lax.axis_index("cand")
    z, x = lax.div(me, NX), lax.rem(me, NX)

    env = lax.axis_index("env")
    core = lax.rem(env, 2)
    relays_two, is_guest = core == 1, core == 0

    def zpeer(d, over=0):
        return {"cand": lax.rem(me + NX * d, E), "env": env + over}

    def xpeer(j, over=0):
        return {"cand": z * NX + lax.rem(x + j, NX), "env": env + over}

    def zback(d):
        return lax.rem(z + NZ - d, NZ)

    def xback(j):
        return lax.rem(x + NX - j, NX)

    def remote(src, dst, send, recv, peer):
        return pltpu.make_async_remote_copy(
            src_ref=src, dst_ref=dst, send_sem=send, recv_sem=recv,
            device_id=peer, device_id_type=pl.DeviceIdType.MESH,
        )

    small = [
        pltpu.make_async_copy(src, dst, load_sem.at[i])
        for i, (src, dst) in enumerate(
            ((mean_hbm, mean_ref), (var_hbm, var_ref), (start_hbm, start_ref),
             (bias_hbm, bias_ref), (elite_hbm, elite_ref), (noise_hbm, noise_v))
        )
    ]
    for c in small[:3]:
        c.start()
    barrier = pltpu.get_barrier_semaphore()

    def greet(peer):
        pl.semaphore_signal(barrier, inc=1, device_id=peer, device_id_type=pl.DeviceIdType.MESH)

    @pl.when(relays_two)
    def _():
        for d in DIRECT[::-1]:
            greet(zpeer(d, -1))
            greet(zpeer(d))

    @pl.when(is_guest)
    def _():
        for j in range(NX):
            greet(xpeer(j, 1))

    for j in range(1, NX):
        greet(xpeer(j))
    for c in small[3:]:
        c.start()

    for c in small[:3]:
        c.wait()
    rows[x, z, :, 0:F] = mean_ref[...]
    rows[x, z, :, F : 2 * F] = jnp.sqrt(var_ref[...])
    rows[x, z, :, 2 * F : ROW] = start_ref[...]

    pl.semaphore_wait(barrier, len(DIRECT) + NX - 1 + NX * core)

    mine = rows.at[x, z]

    @pl.when(relays_two)
    def _():
        for d in DIRECT[::-1]:
            remote(mine, mine, zs, zr.at[d], zpeer(d)).start()

    @pl.when(is_guest)
    def _():
        for d in DIRECT[::-1]:
            remote(mine, guests.at[z], zs, gr.at[d], zpeer(d, 1)).start()

    for j in range(1, NX):
        remote(mine, mine, xs, xr.at[j], xpeer(j)).start()

    for m in range(M):
        pltpu.make_async_copy(wo_hbm.at[m], w2.at[m], load_sem.at[6]).start()
        for r in range(4):
            pltpu.make_async_copy(ws_hbm.at[m], w1.at[m, r, 0:S, :], load_sem.at[7]).start()
            rest = w1.at[m, r, S + ADIM * r : S + ADIM * (r + 1), :]
            pltpu.make_async_copy(wa_hbm.at[m], rest, load_sem.at[7]).start()

    small[4].wait()
    wide[...] = jnp.full((E, 128), -1, jnp.int32)
    wide[:, 0:ELITE] = elite_ref[...]
    for k in range(NX):
        eip[NZ * k : NZ * (k + 1), :] = wide[pl.ds(k, NZ, stride=NX), :]

    small[5].wait()
    for q in range(4):
        part = noise_v[:, :, 128 * q : 128 * (q + 1)]
        noise_f[q] = part.astype(F32).reshape(E * CD, 128)

    for k in range(NX):
        listed = eip[NZ * k : NZ * (k + 1), :]
        before = jnp.zeros((NZ, 1), F32)
        slots = [jnp.zeros((NZ, F), F32) for _ in range(CAP)]
        for c in range(CD):
            hit = jnp.where(listed == me * CD + c, 1.0, 0.0)
            chosen = jnp.sum(hit, axis=1, keepdims=True)
            at = pl.ds(k * CD + c, NZ, stride=NX * CD)
            drawn = jnp.concatenate([noise_f[q, at, :] for q in range(4)], axis=1)
            noise_c[k, c] = drawn
            place = jnp.where(chosen > 0.5, before, -1.0)
            for s in range(min(c + 1, CAP)):
                slots[s] = jnp.where(place == float(s), drawn, slots[s])
            before = before + chosen
        for s in range(CAP):
            elites[k, s] = slots[s].astype(BF)

    for j in range(1, NX):
        remote(elites.at[lax.rem(x + j, NX)], arrived.at[j], ns, nr.at[j], xpeer(j)).start()

    small[3].wait()
    for m in range(M):
        b = bias_ref[m : m + 1, :]
        hi = b.astype(BF).astype(F32)
        mid = (b - hi).astype(BF).astype(F32)
        low = b - hi - mid
        at = lax.broadcasted_iota(jnp.int32, (ADIM, HID), 0)
        tile = jnp.where(at == 0, hi, jnp.where(at == 1, mid, jnp.where(at == 2, low, 0.0)))
        tile = tile.astype(BF)
        for r in range(4):
            for k in range(4):
                if k != r:
                    w1[m, r, S + ADIM * k : S + ADIM * (k + 1), :] = (
                        tile if k == (r + 1) % 4 else jnp.zeros((ADIM, HID), BF)
                    )

    @pl.when(relays_two)
    def _():
        for d in NEAR:
            near = d <= REACH or NZ - REACH < d
            onward = REACH if d <= REACH else NZ - REACH
            far = (d + onward) % NZ
            guest, seat = guests.at[zback(d)], rows.at[x, zback(d)]
            remote(seat, seat, zs, zr.at[d], zpeer(d)).wait_recv()
            if near:
                remote(seat, seat, zs, zr.at[far], zpeer(onward)).start()
            for j in (2, 1, 3):
                remote(seat, seat, xs, xr.at[j], xpeer(j)).start()
            remote(guest, guest, gs.at[1], gr.at[d], zpeer(d)).wait_recv()
            if near:
                remote(guest, guest, gs.at[1], gr.at[far], zpeer(onward)).start()
            for j in (2, 1, 3):
                remote(guest, seat, gs.at[0], xr.at[j], xpeer(j, -1)).start()
            remote(guest, seat, gs.at[1], zr.at[d], xpeer(0, -1)).start()

    @pl.when(is_guest)
    def _():
        for d in NEAR:
            seat = rows.at[x, zback(d)]
            remote(seat, seat, zs, zr.at[d], zpeer(d)).wait_recv()

    own = rows[x].reshape(NZ, ROW)
    line_mean, line_std = own[:, 0:F], own[:, F : 2 * F]
    line_listed = eip[pl.ds(pl.multiple_of(x * NZ, NZ), NZ), :] // CD
    first_sum = jnp.zeros((NZ, F), F32)
    second_sum = jnp.zeros((NZ, F), F32)
    for j in range(NX):
        block = z * NX + xback(j)
        count = jnp.sum(jnp.where(line_listed == block, 1.0, 0.0), axis=1, keepdims=True)
        if j > 0:
            remote(elites.at[0], arrived.at[j], ns, nr.at[j], xpeer(j)).wait_recv()
        for s in range(CAP):
            drawn = (elites[x, s] if j == 0 else arrived[j, s]).astype(F32)
            a = jnp.clip(line_mean + line_std * drawn, -1.0, 1.0).astype(BF).astype(F32)
            a = jnp.where(count > float(s), a, 0.0)
            first_sum = first_sum + a
            second_sum = second_sum + a * a
    for k in range(4):
        cut = slice(128 * k, 128 * (k + 1))
        sums[pl.ds(k, NZ, stride=8), :] = first_sum[:, cut]
        sums[pl.ds(4 + k, NZ, stride=8), :] = second_sum[:, cut]

    for d in NEAR[::-1]:
        remote(
            sums.at[pl.ds(pl.multiple_of(lax.rem(z + d, NZ) * 8, 8), 8), :],
            parts.at[pl.ds(8 * d, 8), :],
            ss, sr, zpeer(d),
        ).start()

    for j in range(NX):
        k = xback(j)
        if j > 0:
            remote(rows.at[k], rows.at[k], xs, xr.at[j], xpeer(j)).wait_recv()
        line = rows[k].reshape(NZ, ROW)
        line_mean, line_std = line[:, 0:F], line[:, F : 2 * F]
        line_start = line[:, 2 * F : ROW]
        initial = -jnp.sum(line_start * line_start, axis=1, keepdims=True)
        for c in range(CD):
            m, h = c % M, c // M
            cut = slice(E * h + NZ * j, E * h + NZ * (j + 1))
            a = jnp.clip(line_mean + line_std * noise_c[k, c], -1.0, 1.0).astype(BF)
            half = a * jnp.asarray(0.5, BF)
            for q in range(4):
                act[m, q, cut, :] = half[:, 128 * q : 128 * (q + 1)]
            a = a.astype(F32)
            asum[m, cut, :] = jnp.sum(a * a, axis=1, keepdims=True)
            states[m, cut, :] = line_start
            energy[m, cut, :] = initial

    pltpu.make_async_copy(wo_hbm, w2, load_sem.at[6]).wait()
    filled = w1.at[:, :, 0 : S + ADIM, :]
    pltpu.make_async_copy(filled, filled, load_sem.at[7]).wait()
    lane = lax.broadcasted_iota(jnp.int32, (2 * E, 128), 1)

    def squares(s):
        return jnp.sum(s * s, axis=1, keepdims=True)

    def step(q, r):
        left = []
        for m in range(M):
            s = states[m]
            e = squares(s)
            energy[m] = energy[m] + e
            n = (s * (0.5 * lax.rsqrt(e * (1.0 / S) + EPSILON))).astype(BF)
            at = ADIM * ((r + 1) % 4)
            ones = jnp.where((lane >= at) & (lane < at + 3), 0.5, 0.0).astype(BF)
            now = (lane >= ADIM * r) & (lane < ADIM * (r + 1))
            left.append((s, jnp.concatenate([n, jnp.where(now, act[m, q], ones)], axis=1)))
        halves = [
            jnp.dot(left[m][1], w1[m, r], preferred_element_type=F32) for m in range(M)
        ]
        for m in range(M):
            h = halves[m]
            hidden = (h + h * jnp.tanh(h)).astype(BF)
            states[m] = left[m][0] + jnp.dot(hidden, w2[m], preferred_element_type=F32)

    def quarter(q, carry):
        for r in range(4):
            step(q, r)
        return carry

    lax.fori_loop(0, 4, quarter, 0)

    out_lane = lax.broadcasted_iota(jnp.int32, (E, 128), 1)
    table = jnp.zeros((E, 128), F32)
    for c in range(CD):
        m, h = c % M, c // M
        cut = slice(E * h, E * (h + 1))
        e = energy[m, cut, :] + squares(states[m, cut, :])
        value = e * (-1.0 / (S * HOR)) - asum[m, cut, :] * (0.1 / (ADIM * HOR))
        table = jnp.where(out_lane == c, value, table)
    for j in range(NX):
        perm[pl.ds(xback(j), NZ, stride=NX), :] = table[NZ * j : NZ * (j + 1), :]
    ret_ref[...] = perm[...].T[0:CD, 0:E]

    others = parts.at[pl.ds(8, 8 * (NZ - 1)), :]
    remote(others, others, ss, sr, zpeer(1)).wait_recv()
    total = sums[pl.ds(pl.multiple_of(z * 8, 8), 8), :]
    for d in range(1, NZ):
        total = total + parts[8 * d : 8 * (d + 1), :]
    for k in range(4):
        cut = slice(128 * k, 128 * (k + 1))
        elite_mean = total[k : k + 1, :] * (1.0 / ELITE)
        elite_var = total[4 + k : 5 + k, :] * (1.0 / ELITE) - elite_mean * elite_mean
        nm_ref[:, cut] = ALPHA * mean_ref[:, cut] + (1.0 - ALPHA) * elite_mean
        nv_ref[:, cut] = ALPHA * var_ref[:, cut] + (1.0 - ALPHA) * elite_var

    remote(others, others, ss, sr, zpeer(1)).wait_send()

    @pl.when(relays_two)
    def _():
        near_and_far = rows.at[0, pl.ds(0, NZ - 1)]
        remote(near_and_far, near_and_far, zs, zr.at[1], zpeer(1)).wait_send()
        sideways = rows.at[pl.ds(0, NX - 1)]
        remote(sideways, sideways, xs, xr.at[1], xpeer(1)).wait_send()
        guests_sideways = rows.at[pl.ds(0, NX - 1), pl.ds(0, NZ - 1)]
        remote(guests_sideways, guests_sideways, gs.at[0], xr.at[1], xpeer(1)).wait_send()
        guests_other = rows.at[pl.ds(0, 2), pl.ds(0, (2 * NZ + REACH * 2 - 2 - NZ) // 2)]
        remote(guests_other, guests_other, gs.at[1], xr.at[1], xpeer(1)).wait_send()

    @pl.when(is_guest)
    def _():
        near = rows.at[0, pl.ds(0, len(DIRECT))]
        remote(near, near, zs, zr.at[1], zpeer(1)).wait_send()
        sideways = rows.at[0, pl.ds(0, NX - 1)]
        remote(sideways, sideways, xs, xr.at[1], xpeer(1)).wait_send()

    sent = arrived.at[pl.ds(1, NX - 1)]
    remote(sent, sent, ns, nr.at[1], xpeer(1)).wait_send()


def put_out(a, b, c, a_out, b_out, c_out, sem):
    copies = [
        pltpu.make_async_copy(src, dst, sem.at[i])
        for i, (src, dst) in enumerate(((a, a_out), (b, b_out), (c, c_out)))
    ]
    for copy in copies:
        copy.start()
    for copy in copies:
        copy.wait()


def per_device(*operands):
    vmem = pl.BlockSpec(memory_space=pltpu.VMEM)
    hbm = pl.BlockSpec(memory_space=pl.ANY)
    dma = pltpu.SemaphoreType.DMA
    shapes = (
            jax.ShapeDtypeStruct((CD, E), F32),
            jax.ShapeDtypeStruct((1, F), F32),
            jax.ShapeDtypeStruct((1, F), F32),
        )
    results = pl.pallas_call(
        kernel,
        out_shape=shapes,
        in_specs=[hbm] * 9,
        out_specs=(vmem, vmem, vmem),
        scratch_shapes=[
            pltpu.VMEM((1, F), F32),
            pltpu.VMEM((1, F), F32),
            pltpu.VMEM((1, S), F32),
            pltpu.VMEM((E, ELITE), jnp.int32),
            pltpu.VMEM((M, HID), F32),
            pltpu.VMEM((NX, NZ, 1, ROW), F32),
            pltpu.VMEM((NZ, 1, ROW), F32),
            pltpu.VMEM((E, CD, F), BF),
            pltpu.VMEM((4, E * CD, 128), F32),
            pltpu.VMEM((NX, CD, NZ, F), F32),
            pltpu.VMEM((E, 128), jnp.int32),
            pltpu.VMEM((E, 128), jnp.int32),
            pltpu.VMEM((NX, CAP, NZ, F), BF),
            pltpu.VMEM((NX, CAP, NZ, F), BF),
            pltpu.VMEM((NZ * 8, 128), F32),
            pltpu.VMEM((NZ * 8, 128), F32),
            pltpu.VMEM((M, 4, 2 * S, HID), BF),
            pltpu.VMEM((M, HID, S), BF),
            pltpu.VMEM((M, 4, 2 * E, 128), BF),
            pltpu.VMEM((M, 2 * E, S), F32),
            pltpu.VMEM((M, 2 * E, 1), F32),
            pltpu.VMEM((M, 2 * E, 1), F32),
            pltpu.VMEM((128, 128), F32),
            dma((8,)), dma((2,)), dma((NZ,)), dma, dma((NZ,)), dma, dma((NX,)), dma, dma((NX,)), dma, dma,
        ],
        compiler_params=pltpu.CompilerParams(
            collective_id=0, has_side_effects=True, vmem_limit_bytes=24 * 2**20
        ),
    )(*(pltpu.with_memory_space_constraint(a, pltpu.HBM) for a in operands))
    returns, new_mean, new_var = pl.pallas_call(
        put_out,
        out_shape=shapes,
        in_specs=[vmem] * 3,
        out_specs=(hbm, hbm, hbm),
        scratch_shapes=[dma((3,))],
        compiler_params=pltpu.CompilerParams(vmem_limit_bytes=24 * 2**20),
    )(*results)
    return returns.T, new_mean, new_var


def solution(mesh):
    both = P(("env", "cand"), None)
    in_specs = (both, both, both, P("env", "cand", None), P("env", None), P(), P(), P(), P())
    return jax.shard_map(
        per_device, mesh=mesh, in_specs=in_specs, out_specs=(P("env", "cand"), both, both),
        check_vma=False,
    )
```
